32 devices in a mesh: dp: 8 (over z, x), tensor: 4 (over y, core).
Axes of the slice: x: 2, y: 2, z: 4, core: 2. Of those that a mesh axis runs over, the one named last changes fastest.
Arguments:
- tokens: bfloat16 [4096, 1536], P(('dp', 'tensor')), may hold values from -6 to 6
- cotangent: bfloat16 [4096, 1536], P(('dp', 'tensor')), may hold values from -6 to 6
- gain_attn: float32 [1536], replicated, may hold values from 0.5 to 1.5
- w_query: bfloat16 [1536, 768], P(None, 'tensor'), may hold values from -0.0546875 to 0.0546875
- w_key: bfloat16 [1536, 768], P(None, 'tensor'), may hold values from -0.0546875 to 0.0546875
- w_value: bfloat16 [1536, 768], P(None, 'tensor'), may hold values from -0.15625 to 0.15625
- w_out: bfloat16 [768, 1536], P('tensor'), may hold values from -3.5 to 3.5
- bias_table: float32 [32, 12], P(None, 'tensor'), may hold values from -4 to 4
- gain_ffn: float32 [1536], replicated, may hold values from 0.5 to 1.5
- w_gate: bfloat16 [1536, 3968], P(None, 'tensor'), may hold values from -0.15625 to 0.15625
- w_up: bfloat16 [1536, 3968], P(None, 'tensor'), may hold values from -0.15625 to 0.15625
- w_down: bfloat16 [3968, 1536], P('tensor'), may hold values from -0.09375 to 0.09375
- lengths: int32 [8, 4], P('dp'), may hold values from 1 to 256, 512 in all within a row
- buckets: int32 [1023], replicated, may hold values from 0 to 31
Outputs:
- block_out: bfloat16 [4096, 1536], P(('dp', 'tensor'))
- grad_tokens: bfloat16 [4096, 1536], P(('dp', 'tensor'))
- grad_gain_attn: float32 [1536], replicated
- grad_w_query: float32 [1536, 768], P(None, 'tensor')
- grad_w_key: float32 [1536, 768], P(None, 'tensor')
- grad_w_value: float32 [1536, 768], P(None, 'tensor')
- grad_w_out: float32 [768, 1536], P('tensor')
- grad_bias_table: float32 [32, 12], P(None, 'tensor')
- grad_gain_ffn: float32 [1536], replicated
- grad_w_gate: float32 [1536, 3968], P(None, 'tensor')
- grad_w_up: float32 [1536, 3968], P(None, 'tensor')
- grad_w_down: float32 [3968, 1536], P('tensor')
The draws below stay inside these ranges and needn't reach their ends.
Inputs may be any that keep to these rules, and one draw needn't show every extreme that they name: `lengths`: each group's 4 rows fill its 512 tokens exactly; in every group the longest row has 256 tokens.
All inputs are finite; a program needn't handle non-finite values.
Results may differ from the reference program's by a relative error of at most 0.017.
Values may be sent and summed in bfloat16 or wider, within the bound.
No kernel may reach another device: no remote copies, remote signals or barrier semaphores. Data moves between devices by JAX's collectives and lax.ppermute only.
A program may use at most 192 MiB of HBM per device.

```python
import math
import jax
import jax.numpy as jnp
import numpy as np
from jax import lax

D = 1536
HEADS = 12
HEAD_DIM = 64
FF = 3968
NB = 32
ROWS = 4
INNER = 768
GRP = 512
LONGEST = 256
GROUPS = 8
TOKENS = 4096
OFFSETS = 1023
N_DP = 8


def place_ends(array, stream_key, low, largest):
    spot = [jax.random.randint(jax.random.fold_in(stream_key, axis), (), 0, length) for axis, length in enumerate(array.shape)]
    widest = array.shape.index(max(array.shape))
    neighbour = spot[:widest] + [(spot[widest] + 1) % array.shape[widest]] + spot[widest + 1:]
    return array.at[tuple(spot)].set(low).at[tuple(neighbour)].set(largest)


def shard_levels(own_key, shape, split, low, top_value):
    level, own = 1.0, jax.random.fold_in(own_key, 6)
    for position, shards_of in split:
        heights = jnp.exp(jax.random.uniform(jax.random.fold_in(own, position), (shards_of,), jnp.float32, low / len(split), top_value / len(split)))
        level = level * jnp.repeat(heights, shape[position] // shards_of).reshape([-1 if axis == position else 1 for axis in range(len(shape))])
    return level


def length_profile(number_of, total, most, lean):
    loads = [(1 << 20) // math.isqrt(standing ** lean) + 1 for standing in range(2, number_of + 1)]
    surplus, counts = total - most - (number_of - 1), [1] * (number_of - 1)
    while surplus > 0:
        candidates = [i for i in range(number_of - 1) if counts[i] < most]
        whole, budget = sum([loads[i] for i in candidates]), surplus
        for i in candidates:
            more = min(most - counts[i], max(1, budget * loads[i] // whole), surplus)
            counts[i] = counts[i] + more
            surplus = surplus - more
    return np.array([most] + counts)


def ragged(stream_key, number_of, total, most, lean):
    if number_of == 2:
        one = jax.random.randint(stream_key, (), max(1, total - most), min(most, total - 1) + 1)
        return jnp.stack([one, total - one])
    tallies = jnp.asarray(length_profile(number_of, total, most, lean), jnp.int32)
    couples = (number_of - 1) // 2
    source_of, receiver = tallies[1:1 + 2 * couples:2], tallies[2:2 + 2 * couples:2]
    margin = jnp.minimum(source_of - 1, most - receiver)
    shifted = jax.random.randint(jax.random.fold_in(stream_key, 1), (couples,), 0, 1 << 20) % (margin + 1)
    tallies = tallies.at[1:1 + 2 * couples:2].set(source_of - shifted).at[2:2 + 2 * couples:2].set(receiver + shifted)
    return tallies[jax.random.permutation(jax.random.fold_in(stream_key, 2), number_of)]


def gaussian(stream_key, dims, spread, limit, pieces=(), kind=jnp.bfloat16):
    array = jax.random.normal(stream_key, dims, jnp.float32) * spread
    if len(pieces) > 0:
        array = shard_levels(stream_key, dims, pieces, -0.22, 0.18) * array
    return jnp.clip(array, min=-limit, max=limit).astype(kind)


def setup_inputs(seed: int = 0) -> dict:
    arg_keys = jax.random.split(jax.random.key(seed), 15)
    tokens = gaussian(arg_keys[0], (TOKENS, D), 1.0, 6.0, ((0, 32),))
    cotangent = gaussian(arg_keys[1], (TOKENS, D), 1.0, 6.0, ((0, 32),))
    gain_attn = jnp.clip(1.0 + 0.1 * jax.random.normal(arg_keys[2], (D,), jnp.float32), 0.5, 1.5)
    w_query = gaussian(arg_keys[3], (D, INNER), (8 * D) ** -0.5, 0.0546875, ((1, 4),))
    w_key = gaussian(arg_keys[4], (D, INNER), (8 * D) ** -0.5, 0.0546875, ((1, 4),))
    w_value = gaussian(arg_keys[5], (D, INNER), D ** -0.5, 0.15625, ((1, 4),))
    w_out = gaussian(arg_keys[6], (INNER, D), (max(INNER // 256, 1)) ** -0.5, 3.5, ((0, 4),))
    bias_table = gaussian(arg_keys[7], (NB, HEADS), 1.0, 4.0, ((1, 4),), jnp.float32)
    gain_ffn = jnp.clip(1.0 + 0.1 * jax.random.normal(arg_keys[8], (D,), jnp.float32), 0.5, 1.5)
    w_gate = gaussian(arg_keys[9], (D, FF), D ** -0.5, 0.15625, ((1, 4),))
    w_up = gaussian(arg_keys[10], (D, FF), D ** -0.5, 0.15625, ((1, 4),))
    w_down = gaussian(arg_keys[11], (FF, D), FF ** -0.5, 0.09375, ((0, 4),))
    lengths = jax.vmap(lambda own: ragged(own, ROWS, GRP, LONGEST, 2))(jax.random.split(arg_keys[12], GROUPS)).reshape((GROUPS, ROWS)).astype(jnp.int32)
    buckets = place_ends(jax.random.randint(arg_keys[13], (OFFSETS,), 0, NB), jax.random.fold_in(arg_keys[13], 1), 0, NB - 1).astype(jnp.int32)
    return {"tokens": tokens, "cotangent": cotangent, "gain_attn": gain_attn, "w_query": w_query, "w_key": w_key, "w_value": w_value, "w_out": w_out, "bias_table": bias_table, "gain_ffn": gain_ffn, "w_gate": w_gate, "w_up": w_up, "w_down": w_down, "lengths": lengths, "buckets": buckets}


@jax.custom_vjp
def low(v):
    return lax.optimization_barrier(v.astype(jnp.bfloat16)).astype(jnp.float32)

@jax.custom_vjp
def low_back(v):
    return v

def low_keep(v):
    return (low(v), None)

def low_pass(kept, grad):
    return (grad,)

def back_keep(v):
    return (v, None)

def back_low(kept, grad):
    return (low(grad),)
low.defvjp(low_keep, low_pass)
low_back.defvjp(back_keep, back_low)

def matmul(left, right):
    return jnp.dot(left, right, precision=lax.Precision.HIGHEST)

def rms_norm(value, gain):
    return value * lax.rsqrt(lax.optimization_barrier(jnp.mean(value * value, axis=-1, keepdims=True)) + 1e-06) * gain

def segment_ids(row_lengths):
    ends = jnp.cumsum(row_lengths)
    place = jnp.arange(GRP, dtype=jnp.int32)
    return lax.optimization_barrier(jnp.sum((place[:, None] >= ends[None, :-1]).astype(jnp.int32), axis=1))

def group_attention(query, keys, values, row_id, table, bucket_grid):
    bias = jnp.moveaxis(table[bucket_grid], 2, 0)
    scores = jnp.einsum('qhd,khd->hqk', query, keys, precision=lax.Precision.HIGHEST) + bias
    scores = low_back(scores)
    same = row_id[:, None] == row_id[None, :]
    scores = jnp.where(same[None], scores, -1e+30)
    probability = jax.nn.softmax(scores, axis=-1)
    result = jnp.einsum('hqk,khd->qhd', low(probability), values, precision=lax.Precision.HIGHEST)
    return low(low_back(result))

def reference(tokens, cotangent, gain_attn, w_query, w_key, w_value, w_out, bias_table, gain_ffn, w_gate, w_up, w_down, lengths, buckets):
    row_ids = jax.vmap(segment_ids)(lengths)
    place = jnp.arange(GRP, dtype=jnp.int32)
    bucket_grid = buckets[place[None, :] - place[:, None] + (GRP - 1)]

    def forward(source, gain_first, query_proj, key_proj, value_proj, out_proj, table, gain_second, gate_proj, up_proj, down_proj):
        normed_one = low(rms_norm(source, gain_first))
        query = low(low_back(matmul(normed_one, query_proj)))
        keys = low(low_back(matmul(normed_one, key_proj)))
        values = low(low_back(matmul(normed_one, value_proj)))
        shape = (N_DP, GRP, HEADS, HEAD_DIM)

        def one_group(items):
            return group_attention(items[0], items[1], items[2], items[3], table, bucket_grid)
        attended = lax.map(jax.checkpoint(one_group), (query.reshape(shape), keys.reshape(shape), values.reshape(shape), row_ids))
        attention = attended.reshape(TOKENS, INNER)
        middle = source + low_back(matmul(attention, out_proj))
        normed_two = low(rms_norm(middle, gain_second))
        gate = low_back(matmul(normed_two, gate_proj))
        up_value = low_back(matmul(normed_two, up_proj))
        hidden = low(jax.nn.gelu(gate, approximate=True) * up_value)
        return middle + matmul(hidden, down_proj)
    inputs = (tokens.astype(jnp.float32), gain_attn, w_query.astype(jnp.float32), w_key.astype(jnp.float32), w_value.astype(jnp.float32), w_out.astype(jnp.float32), bias_table, gain_ffn, w_gate.astype(jnp.float32), w_up.astype(jnp.float32), w_down.astype(jnp.float32))
    result, pullback = jax.vjp(forward, *inputs)
    grads = pullback(cotangent.astype(jnp.float32))
    return (result.astype(jnp.bfloat16), grads[0].astype(jnp.bfloat16), grads[1], grads[2], grads[3], grads[4], grads[5], grads[6], grads[7], grads[8], grads[9], grads[10])
```

```python
import functools

import jax
import jax.numpy as jnp
from jax import lax
from jax.experimental import pallas as pl
from jax.experimental.pallas import tpu as pltpu
from jax.sharding import PartitionSpec as P

F32 = jnp.float32
BF16 = jnp.bfloat16
ORDER = (0, 2, 1, 3)


def swap_bits(index):
    return ((index & 1) << 1) | (index >> 1)


def dot_nn(left, right):
    return lax.dot_general(left, right, (((1,), (0,)), ((), ())), preferred_element_type=F32)


def dot_tn(left, right):
    return lax.dot_general(left, right, (((0,), (0,)), ((), ())), preferred_element_type=F32)


def dot_nt(left, right):
    return lax.dot_general(left, right, (((1,), (1,)), ((), ())), preferred_element_type=F32)


def attn_forward_kernel(
    place_ref, lens_ref, table_ref, buckets_ref, qkv_ref, attn_ref, prob_ref, tiles_ref, *, heads, size, blk, nblk
):
    step = pl.program_id(0)
    place = place_ref[0]
    inner = heads * size

    @pl.when(step == 0)
    def _():
        buckets = buckets_ref[...]
        for h in range(heads):
            vec = jnp.zeros(buckets.shape, F32)
            for b in range(table_ref.shape[0]):
                vec = jnp.where(buckets == b, table_ref[b, h], vec)
            for d in range(2 * nblk - 1):
                seg = jnp.broadcast_to(vec[:, d * blk : (d + 2) * blk], (blk, 2 * blk))
                tiles_ref[h, d] = pltpu.roll(seg, blk, 1, stride=1, stride_axis=0)[:, :blk]

    def row_of(pos):
        row, end = jnp.zeros(pos.shape, jnp.int32), jnp.int32(0)
        for r in range(lens_ref.shape[1] - 1):
            end = end + lens_ref[0, r]
            row = row + (pos >= end).astype(jnp.int32)
        return row

    here = place ^ swap_bits(step)
    row_q = row_of(here * blk + lax.broadcasted_iota(jnp.int32, (blk, 1), 0))
    lane = lax.broadcasted_iota(jnp.int32, (1, blk), 1)
    row_k = jnp.concatenate([row_of((place ^ m) * blk + lane) for m in ORDER], axis=1)
    same = row_q == row_k
    rows = pl.ds(step * blk, blk)
    for h in range(heads):
        query = qkv_ref[rows, h * size : (h + 1) * size]
        keys = qkv_ref[:, inner + h * size : inner + (h + 1) * size]
        values = qkv_ref[:, 2 * inner + h * size : 2 * inner + (h + 1) * size]
        bias = jnp.concatenate([tiles_ref[h, (place ^ m) - here + nblk - 1] for m in ORDER], axis=1)
        scores = jnp.where(same, dot_nt(query, keys) + bias, -1e30)
        raised = jnp.exp(scores - jnp.max(scores, axis=1, keepdims=True))
        prob = (raised * (1.0 / jnp.sum(raised, axis=1, keepdims=True))).astype(BF16)
        prob_ref[h] = prob
        attn_ref[:, h * size : (h + 1) * size] = dot_nn(prob, values).astype(BF16)


def attn_forward(place, lens, table, buckets, qkv, heads, size, blk):
    count = qkv.shape[0]
    nblk = count // blk
    return pl.pallas_call(
        functools.partial(attn_forward_kernel, heads=heads, size=size, blk=blk, nblk=nblk),
        out_shape=(
            jax.ShapeDtypeStruct((count, heads * size), BF16),
            jax.ShapeDtypeStruct((heads, count, count), BF16),
        ),
        grid_spec=pltpu.PrefetchScalarGridSpec(
            num_scalar_prefetch=3,
            grid=(nblk,),
            in_specs=[
                pl.BlockSpec(buckets.shape, lambda i, *_: (0, 0)),
                pl.BlockSpec(qkv.shape, lambda i, *_: (0, 0)),
            ],
            out_specs=[
                pl.BlockSpec((blk, heads * size), lambda i, *_: (i, 0)),
                pl.BlockSpec((heads, blk, count), lambda i, *_: (0, i, 0)),
            ],
            scratch_shapes=[pltpu.VMEM((heads, 2 * nblk - 1, blk, blk), F32)],
        ),
        cost_estimate=pl.CostEstimate(flops=8 * heads * count * count * size, bytes_accessed=4 * heads * count * count, transcendentals=heads * count * count),
        name="attn_forward",
    )(place, lens, table, buckets, qkv)


def attn_backward_kernel(
    place_ref, buckets_ref, qkv_ref, grad_ref, prob_ref, gqkv_ref, gtable_ref, dk_ref, dv_ref, tiles_ref, vec_ref,
    *, heads, size, blk, nblk, bins
):
    step = pl.program_id(0)
    place = place_ref[0]
    inner = heads * size

    @pl.when(step == 0)
    def _():
        dk_ref[...] = jnp.zeros_like(dk_ref)
        dv_ref[...] = jnp.zeros_like(dv_ref)
        tiles_ref[...] = jnp.zeros_like(tiles_ref)

    here = place ^ swap_bits(step)
    rows = pl.ds(step * blk, blk)
    for h in range(heads):
        query = qkv_ref[rows, h * size : (h + 1) * size]
        keys = qkv_ref[:, inner + h * size : inner + (h + 1) * size]
        values = qkv_ref[:, 2 * inner + h * size : 2 * inner + (h + 1) * size]
        grad = grad_ref[rows, h * size : (h + 1) * size]
        prob_low = prob_ref[h]
        prob = prob_low.astype(F32)
        grad_prob = dot_nt(grad, values)
        delta = jnp.sum(prob * grad_prob, axis=1, keepdims=True)
        grad_scores = (prob * (grad_prob - delta)).astype(BF16)
        dv_ref[h] += dot_tn(prob_low, grad)
        dk_ref[h] += dot_tn(grad_scores, query)
        gqkv_ref[rows, h * size : (h + 1) * size] = dot_nn(grad_scores, keys).astype(BF16)
        for b, m in enumerate(ORDER):
            tiles_ref[h, (place ^ m) - here + nblk - 1] += grad_scores[:, b * blk : (b + 1) * blk].astype(F32)

    @pl.when(step == nblk - 1)
    def _():
        vec_ref[...] = jnp.zeros_like(vec_ref)
        back = (
            lax.broadcasted_iota(jnp.int32, (blk, blk), 0) + lax.broadcasted_iota(jnp.int32, (blk, blk), 1) == blk - 1
        ).astype(F32)
        for h in range(heads):
            gqkv_ref[:, inner + h * size : inner + (h + 1) * size] = dk_ref[h].astype(BF16)
            gqkv_ref[:, 2 * inner + h * size : 2 * inner + (h + 1) * size] = dv_ref[h].astype(BF16)
            for d in range(2 * nblk - 1):
                flip = jnp.dot(back, tiles_ref[h, d], precision=lax.Precision.HIGHEST, preferred_element_type=F32)
                wide = jnp.concatenate([flip, jnp.zeros((blk, blk), F32)], axis=1)
                moved = pltpu.roll(wide, 1, 1, stride=1, stride_axis=0)
                vec_ref[h : h + 1, d * blk : (d + 2) * blk] += jnp.sum(moved, axis=0, keepdims=True)
        pick = (lax.broadcasted_iota(jnp.int32, (bins, 1), 0) == buckets_ref[...]).astype(F32)
        gtable_ref[...] = lax.dot_general(
            pick, vec_ref[...], (((1,), (1,)), ((), ())), precision=lax.Precision.HIGHEST, preferred_element_type=F32
        )


def attn_backward(place, buckets, qkv, grad, prob, heads, size, blk, bins):
    count = qkv.shape[0]
    nblk = count // blk
    whole = lambda i, *_: (0, 0)
    return pl.pallas_call(
        functools.partial(attn_backward_kernel, heads=heads, size=size, blk=blk, nblk=nblk, bins=bins),
        out_shape=(jax.ShapeDtypeStruct(qkv.shape, BF16), jax.ShapeDtypeStruct((bins, 8), F32)),
        grid_spec=pltpu.PrefetchScalarGridSpec(
            num_scalar_prefetch=1,
            grid=(nblk,),
            in_specs=[
                pl.BlockSpec(buckets.shape, whole),
                pl.BlockSpec(qkv.shape, whole),
                pl.BlockSpec(grad.shape, whole),
                pl.BlockSpec((heads, blk, count), lambda i, *_: (0, i, 0)),
            ],
            out_specs=[pl.BlockSpec(qkv.shape, whole), pl.BlockSpec((bins, 8), whole)],
            scratch_shapes=[
                pltpu.VMEM((heads, count, size), F32),
                pltpu.VMEM((heads, count, size), F32),
                pltpu.VMEM((heads, 2 * nblk - 1, blk, blk), F32),
                pltpu.VMEM((8, 2 * nblk * blk), F32),
            ],
        ),
        cost_estimate=pl.CostEstimate(flops=10 * heads * count * count * size, bytes_accessed=4 * heads * count * count, transcendentals=0),
        name="attn_backward",
    )(place, buckets, qkv, grad, prob)


def after(value, *gates):
    return lax.optimization_barrier((value, *gates))[0]


def body(
    tokens, cotangent, gain_attn, w_query, w_key, w_value, w_out, bias_table, gain_ffn, w_gate, w_up, w_down, lengths, buckets,
):
    n_t, n_d = lax.axis_size("tensor"), lax.axis_size("dp")
    blk, width = tokens.shape
    heads = bias_table.shape[1]
    inner = w_query.shape[1]
    size = inner // heads
    bins = bias_table.shape[0]
    t_at, d_at = lax.axis_index("tensor"), lax.axis_index("dp")
    x_at, z_at, n_z = d_at & 1, d_at >> 1, n_d // 2

    def tensor_swap(value, mask):
        return lax.ppermute(value, "tensor", [(i, i ^ mask) for i in range(n_t)])

    def dp_swap(value, mask):
        return lax.ppermute(value, "dp", [(i, i ^ mask) for i in range(n_d)])

    def z_send(value, pairs):
        return lax.ppermute(value, "dp", [(2 * a + x, 2 * b + x) for a, b in pairs for x in (0, 1)])

    def z_sum(value):
        if n_z == 4:
            value = value + z_send(value, ((0, 1), (3, 2)))
            value = value + z_send(value, ((1, 2), (2, 1)))
            ends = z_send(value, ((1, 0), (2, 3)))
            return jnp.where((z_at == 0) | (z_at == 3), ends, value)
        step = 2
        while step < n_d:
            value = value + dp_swap(value, step)
            step *= 2
        return value

    def in_order(mine, other):
        first = x_at == 0
        return jnp.where(first, mine, other), jnp.where(first, other, mine)

    tok_y = tensor_swap(tokens, 2)
    tok_c = tensor_swap(tokens, 1)
    tok_yc = tensor_swap(tok_y, 1)
    tok_all = jnp.concatenate([tokens, tok_y, tok_c, tok_yc], axis=0).astype(F32)
    rr1_all = lax.rsqrt(jnp.mean(tok_all * tok_all, axis=1, keepdims=True) + 1e-6)
    n1 = (tok_all * rr1_all * gain_attn).astype(BF16)

    w_qkv = jnp.concatenate([w_query, w_key, w_value], axis=1)
    qkv = dot_nn(n1, w_qkv).astype(BF16)

    wo_own = after(w_out, tok_y)
    wo_y = tensor_swap(wo_own, 2)
    wo_c = tensor_swap(wo_own, 1)
    wo_yc = tensor_swap(wo_y, 1)
    wo_all = jnp.concatenate([w_out, wo_y, wo_c, wo_yc], axis=0)

    def gather8(value):
        from_y = tensor_swap(value, 2)
        from_x = dp_swap(value, 1)
        half = blk // 2
        diag = jnp.concatenate([tensor_swap(from_x[:half], 2), dp_swap(from_y[half:], 1)], axis=0)
        near = jnp.concatenate([value, from_x, from_y, diag], axis=0)
        return jnp.concatenate([near, tensor_swap(near, 1)], axis=0)

    def scatter8(near, far):
        near = near + tensor_swap(far, 1)
        near = near[: 2 * blk] + tensor_swap(near[2 * blk :], 2)
        return near[:blk].astype(F32) + dp_swap(near[blk:], 1).astype(F32)

    def scatter4(near, far):
        near = near + tensor_swap(far, 1)
        return near[:blk].astype(F32) + tensor_swap(near[blk:], 2).astype(F32)

    cot_all = gather8(after(cotangent, tok_y))

    place = t_at.astype(jnp.int32).reshape(1)
    bucket_row = jnp.pad(buckets, (1, 0), constant_values=-1).reshape(1, -1)
    attn, prob = attn_forward(place, lengths, bias_table, bucket_row, qkv, heads, size, blk)

    def to_owners(blocks):
        return [blocks[0]] + [tensor_swap(blocks[b], ORDER[b]) for b in range(1, n_t)]

    mine = to_owners([attn[b * blk : (b + 1) * blk] for b in range(n_t)])
    tok = tokens.astype(F32)
    y1 = tok + dot_nn(jnp.concatenate(mine, axis=1), wo_all)
    rr2 = lax.rsqrt(jnp.mean(y1 * y1, axis=1, keepdims=True) + 1e-6)
    n2 = (y1 * rr2 * gain_ffn).astype(BF16)
    n2_all = gather8(n2)

    units = w_down.shape[0]
    half = -(-units // 256) * 128
    spare = 2 * half - units
    wg = lax.dynamic_slice_in_dim(jnp.pad(w_gate, ((0, 0), (0, spare))), x_at * half, half, 1)
    wu = lax.dynamic_slice_in_dim(jnp.pad(w_up, ((0, 0), (0, spare))), x_at * half, half, 1)
    wd = lax.dynamic_slice_in_dim(jnp.pad(w_down, ((0, spare), (0, 0))), x_at * half, half, 0)

    grad_hidden = dot_nt(cot_all, wd)
    gate = dot_nn(n2_all, wg)
    up = dot_nn(n2_all, wu)

    def gated(g, u):
        return jax.nn.gelu(g, approximate=True) * u

    hidden_f, pull = jax.vjp(gated, gate, up)
    hidden = hidden_f.astype(BF16)
    gg_f, gu_f = pull(grad_hidden)
    gg, gu = gg_f.astype(BF16), gu_f.astype(BF16)

    def spread(value, parts):
        rows = value.shape[0] // parts
        done = [z_sum(value[i * rows : (i + 1) * rows]) for i in range(parts)]
        both = [in_order(piece, dp_swap(piece, 1)) for piece in done]
        return [b[0] for b in both], [b[1] for b in both]

    down_a, down_b = spread(dot_tn(hidden, cot_all).astype(BF16), 2)
    out_w_down = jnp.concatenate(down_a + down_b, axis=0)[:units].astype(F32)
    gate_a, gate_b = spread(dot_tn(n2_all, gg).astype(BF16), 2)
    out_w_gate = jnp.concatenate([jnp.concatenate(gate_a, 0), jnp.concatenate(gate_b, 0)[:, : units - half]], 1).astype(F32)
    up_a, up_b = spread(dot_tn(n2_all, gu).astype(BF16), 2)
    out_w_up = jnp.concatenate([jnp.concatenate(up_a, 0), jnp.concatenate(up_b, 0)[:, : units - half]], 1).astype(F32)

    side = n_t * blk
    gn2_part = (dot_nt(gg, wg) + dot_nt(gu, wu)).astype(BF16)
    gn2 = scatter8(gn2_part[:side], gn2_part[side:])
    ffn_part = dot_nn(hidden, wd).astype(BF16)
    block_out = (y1 + scatter8(ffn_part[:side], ffn_part[side:])).astype(BF16)

    gain2_part = jnp.sum(gn2 * y1 * rr2, axis=0)
    c2 = gn2 * gain_ffn
    gy1 = cotangent.astype(F32) + rr2 * c2 - y1 * (rr2 * rr2 * rr2) * jnp.mean(c2 * y1, axis=1, keepdims=True)
    gy1_low = gy1.astype(BF16)
    ga_mine = dot_nt(gy1_low, wo_all).astype(BF16)
    ga = jnp.concatenate(to_owners([ga_mine[:, b * inner : (b + 1) * inner] for b in range(n_t)]), axis=0)

    gqkv, gtable = attn_backward(place, bucket_row, qkv, ga, prob, heads, size, blk, bins)

    gy_own = after(gy1_low, ga)
    gy_y = tensor_swap(gy_own, 2)
    gy_near = jnp.concatenate([gy_own, gy_y], axis=0)
    gy_all = jnp.concatenate([gy_near, tensor_swap(gy_near, 1)], axis=0)

    def full_sum(value):
        rows = value.shape[0] // 2
        give = lax.dynamic_slice_in_dim(value, (1 - x_at) * rows, rows, 0)
        keep = lax.dynamic_slice_in_dim(value, x_at * rows, rows, 0)
        piece = z_sum(keep + dp_swap(give, 1))
        return jnp.concatenate(in_order(piece, dp_swap(piece, 1)), axis=0)

    out_w_out = full_sum(dot_tn(attn, gy_all).astype(BF16)).astype(F32)
    g_wqkv = full_sum(dot_tn(n1, gqkv).astype(BF16)).astype(F32)
    gn1_part = dot_nt(gqkv, w_qkv).astype(BF16)
    gn1 = scatter4(gn1_part[: 2 * blk], gn1_part[2 * blk :])

    rr1 = lax.rsqrt(jnp.mean(tok * tok, axis=1, keepdims=True) + 1e-6)
    gain1_part = jnp.sum(gn1 * tok * rr1, axis=0)
    c1 = gn1 * gain_attn
    grad_tokens = (gy1 + rr1 * c1 - tok * (rr1 * rr1 * rr1) * jnp.mean(c1 * tok, axis=1, keepdims=True)).astype(BF16)

    small = jnp.concatenate([gain1_part, gain2_part])
    step = 1
    while step < n_t:
        small = small + tensor_swap(small, step)
        step *= 2
    small = jnp.concatenate([small, gtable.reshape(-1)])
    step = 1
    while step < n_d:
        small = small + dp_swap(small, step)
        step *= 2
    gain1_sum, gain2_sum = small[:width], small[width : 2 * width]
    table_sum = small[2 * width :].reshape(gtable.shape)[:, :heads]

    return (
        block_out,
        grad_tokens,
        gain1_sum,
        g_wqkv[:, :inner],
        g_wqkv[:, inner : 2 * inner],
        g_wqkv[:, 2 * inner :],
        out_w_out,
        table_sum,
        gain2_sum,
        out_w_gate,
        out_w_up,
        out_w_down,
    )


def solution(mesh):
    rows, cols, both = P("tensor", None), P(None, "tensor"), P(("dp", "tensor"), None)
    return jax.shard_map(
        body,
        mesh=mesh,
        in_specs=(both, both, P(), cols, cols, cols, rows, cols, P(), cols, cols, rows, P("dp", None), P()),
        out_specs=(both, both, P(), cols, cols, cols, rows, cols, P(), cols, cols, rows),
        check_vma=False,
    )
```

```python
import functools

import jax
import jax.numpy as jnp
from jax import lax
from jax.experimental import pallas as pl
from jax.experimental.pallas import tpu as pltpu
from jax.sharding import PartitionSpec as P

F32 = jnp.float32
BF16 = jnp.bfloat16
ORDER = (0, 2, 1, 3)


def swap_bits(index):
    return ((index & 1) << 1) | (index >> 1)


def dot_nn(left, right):
    return lax.dot_general(left, right, (((1,), (0,)), ((), ())), preferred_element_type=F32)


def dot_tn(left, right):
    return lax.dot_general(left, right, (((0,), (0,)), ((), ())), preferred_element_type=F32)


def dot_nt(left, right):
    return lax.dot_general(left, right, (((1,), (1,)), ((), ())), preferred_element_type=F32)


def front_kernel(
    place_ref, lens_ref, table_ref, buckets_ref, gain_ref, tok0, tok1, tok2, tok3, wq_ref, wk_ref, wv_ref,
    n1_ref, qkv_ref, prob_ref, out0, out1, out2, out3, tiles_ref, *, heads, size, blk, nblk
):
    step = pl.program_id(0)
    place = place_ref[0]
    inner = heads * size

    @pl.when(step == 0)
    def _():
        buckets = buckets_ref[...]
        for h in range(heads):
            vec = jnp.zeros(buckets.shape, F32)
            for b in range(table_ref.shape[0]):
                vec = jnp.where(buckets == b, table_ref[b, h], vec)
            for d in range(2 * nblk - 1):
                seg = jnp.broadcast_to(vec[:, d * blk : (d + 2) * blk], (blk, 2 * blk))
                tiles_ref[h, d] = pltpu.roll(seg, blk, 1, stride=1, stride_axis=0)[:, :blk]
        for b, ref in enumerate((tok0, tok1, tok2, tok3)):
            tok = ref[...].astype(F32)
            rr = lax.rsqrt(jnp.mean(tok * tok, axis=1, keepdims=True) + 1e-6)
            n1_ref[b * blk : (b + 1) * blk, :] = (tok * rr * gain_ref[...]).astype(BF16)
        n1 = n1_ref[...]
        for i, ref in enumerate((wq_ref, wk_ref, wv_ref)):
            qkv_ref[:, i * inner : (i + 1) * inner] = dot_nn(n1, ref[...]).astype(BF16)

    def row_of(pos):
        row, end = jnp.zeros(pos.shape, jnp.int32), jnp.int32(0)
        for r in range(lens_ref.shape[1] - 1):
            end = end + lens_ref[0, r]
            row = row + (pos >= end).astype(jnp.int32)
        return row

    here = place ^ swap_bits(step)
    row_q = row_of(here * blk + lax.broadcasted_iota(jnp.int32, (blk, 1), 0))
    lane = lax.broadcasted_iota(jnp.int32, (1, blk), 1)
    row_k = jnp.concatenate([row_of((place ^ m) * blk + lane) for m in ORDER], axis=1)
    same = row_q == row_k
    rows = pl.ds(step * blk, blk)
    outs = []
    for h in range(heads):
        query = qkv_ref[rows, h * size : (h + 1) * size]
        keys = qkv_ref[:, inner + h * size : inner + (h + 1) * size]
        values = qkv_ref[:, 2 * inner + h * size : 2 * inner + (h + 1) * size]
        bias = jnp.concatenate([tiles_ref[h, (place ^ m) - here + nblk - 1] for m in ORDER], axis=1)
        scores = jnp.where(same, dot_nt(query, keys) + bias, -1e30)
        raised = jnp.exp(scores - jnp.max(scores, axis=1, keepdims=True))
        prob = (raised * (1.0 / jnp.sum(raised, axis=1, keepdims=True))).astype(BF16)
        prob_ref[h] = prob
        outs.append(dot_nn(prob, values).astype(BF16))
    joined = jnp.concatenate(outs, axis=1)
    for b, ref in enumerate((out0, out1, out2, out3)):

        @pl.when(step == b)
        def _(ref=ref):
            ref[...] = joined


def front(place, lens, table, buckets, gain, toks, wq, wk, wv, heads, size):
    blk, width = toks[0].shape
    nblk = len(toks)
    count = nblk * blk
    inner = heads * size
    whole = lambda i, *_: (0, 0)
    return pl.pallas_call(
        functools.partial(front_kernel, heads=heads, size=size, blk=blk, nblk=nblk),
        out_shape=(
            jax.ShapeDtypeStruct((count, width), BF16),
            jax.ShapeDtypeStruct((count, 3 * inner), BF16),
            jax.ShapeDtypeStruct((heads, count, count), BF16),
        )
        + tuple(jax.ShapeDtypeStruct((blk, inner), BF16) for _ in range(nblk)),
        grid_spec=pltpu.PrefetchScalarGridSpec(
            num_scalar_prefetch=3,
            grid=(nblk,),
            in_specs=[pl.BlockSpec(a.shape, whole) for a in (buckets, gain, *toks, wq, wk, wv)],
            out_specs=[
                pl.BlockSpec((count, width), whole),
                pl.BlockSpec((count, 3 * inner), whole),
                pl.BlockSpec((heads, blk, count), lambda i, *_: (0, i, 0)),
            ]
            + [pl.BlockSpec((blk, inner), whole) for _ in range(nblk)],
            scratch_shapes=[pltpu.VMEM((heads, 2 * nblk - 1, blk, blk), F32)],
        ),
        cost_estimate=pl.CostEstimate(
            flops=6 * count * width * inner + 4 * count * count * inner,
            bytes_accessed=4 * count * width + 6 * width * inner + 2 * heads * count * count,
            transcendentals=heads * count * count,
        ),
        name="front",
    )(place, lens, table, buckets, gain, *toks, wq, wk, wv)


def middle_kernel(a0, a1, a2, a3, w0, w1, w2, w3, tok_ref, gain_ref, y1_ref, n2_ref):
    y1 = tok_ref[...].astype(F32)
    for a, w in ((a0, w0), (a1, w1), (a2, w2), (a3, w3)):
        y1 = y1 + dot_nn(a[...], w[...])
    rr = lax.rsqrt(jnp.mean(y1 * y1, axis=1, keepdims=True) + 1e-6)
    y1_ref[...] = y1
    n2_ref[...] = (y1 * rr * gain_ref[...]).astype(BF16)


def middle(attns, wos, tok, gain):
    return pl.pallas_call(
        middle_kernel,
        out_shape=(jax.ShapeDtypeStruct(tok.shape, F32), jax.ShapeDtypeStruct(tok.shape, BF16)),
        cost_estimate=pl.CostEstimate(flops=8 * tok.shape[0] * tok.shape[1] * wos[0].shape[0], bytes_accessed=8 * wos[0].size + 8 * tok.size, transcendentals=0),
        name="middle",
    )(*attns, *wos, tok, gain)


SQ = 0.7978845608028654


def ffn_kernel(n0, n1, n2, n3, n4, n5, n6, n7, cot_ref, wg_ref, wu_ref, wd_ref, hid_ref, gg_ref, gu_ref, all_ref, *, blk):
    @pl.when(pl.program_id(0) == 0)
    def _():
        for b, ref in enumerate((n0, n1, n2, n3, n4, n5, n6, n7)):
            all_ref[b * blk : (b + 1) * blk, :] = ref[...]

    rows = all_ref.shape[0] // 4

    def part(i, carry):
        at = pl.ds(pl.multiple_of(i * rows, rows), rows)
        gate = dot_nn(all_ref[at, :], wg_ref[...])
        up = dot_nn(all_ref[at, :], wu_ref[...])
        grad = dot_nt(cot_ref[at, :], wd_ref[...])
        square = gate * gate
        tanh = jnp.tanh(SQ * gate * (1.0 + 0.044715 * square))
        half = 0.5 * (1.0 + tanh)
        gelu = gate * half
        slope = half + 0.5 * gate * (1.0 - tanh * tanh) * (SQ * (1.0 + 3 * 0.044715 * square))
        hid_ref[at, :] = (gelu * up).astype(BF16)
        gg_ref[at, :] = (grad * up * slope).astype(BF16)
        gu_ref[at, :] = (grad * gelu).astype(BF16)
        return carry

    lax.fori_loop(0, 4, part, 0)


def ffn(blocks, cot, wg, wu, wd, tile=256):
    blk, width = blocks[0].shape
    count, half = blk * len(blocks), wg.shape[1]
    whole = lambda j: (0, 0)
    col = lambda j: (0, j)
    return pl.pallas_call(
        functools.partial(ffn_kernel, blk=blk),
        grid=(half // tile,),
        out_shape=tuple(jax.ShapeDtypeStruct((count, half), BF16) for _ in range(3)) + (jax.ShapeDtypeStruct((count, width), BF16),),
        in_specs=[pl.BlockSpec((blk, width), whole) for _ in blocks]
        + [
            pl.BlockSpec((count, width), whole),
            pl.BlockSpec((width, tile), col),
            pl.BlockSpec((width, tile), col),
            pl.BlockSpec((tile, width), lambda j: (j, 0)),
        ],
        out_specs=[pl.BlockSpec((count, tile), col) for _ in range(3)] + [pl.BlockSpec((count, width), whole)],
        cost_estimate=pl.CostEstimate(flops=6 * count * width * half, bytes_accessed=6 * count * width + 6 * width * half + 6 * count * half, transcendentals=count * half),
        name="ffn",
    )(*blocks, cot, wg, wu, wd)


def back_kernel(near_ref, got_ref, y1_ref, cot_ref, gain_ref, w0, w1, w2, w3, gy_ref, low_ref, sum_ref, g0, g1, g2, g3):
    gn2 = near_ref[...].astype(F32) + got_ref[...].astype(F32)
    y1 = y1_ref[...]
    rr = lax.rsqrt(jnp.mean(y1 * y1, axis=1, keepdims=True) + 1e-6)
    sum_ref[...] = jnp.sum(gn2 * y1 * rr, axis=0, keepdims=True)
    c2 = gn2 * gain_ref[...]
    gy = cot_ref[...].astype(F32) + rr * c2 - y1 * (rr * rr * rr * jnp.mean(c2 * y1, axis=1, keepdims=True))
    gy_ref[...] = gy
    low = gy.astype(BF16)
    low_ref[...] = low
    for w, g in ((w0, g0), (w1, g1), (w2, g2), (w3, g3)):
        g[...] = dot_nt(low, w[...]).astype(BF16)


def back(near, got, y1, cot, gain, wos):
    blk, width = y1.shape
    inner = wos[0].shape[0]
    return pl.pallas_call(
        back_kernel,
        grid=(1,),
        in_specs=[
            pl.BlockSpec((blk, width), lambda i: (0, 0)),
            pl.BlockSpec((blk, width), lambda i: (0, 0)),
            pl.BlockSpec((blk, width), lambda i: (0, 0)),
            pl.BlockSpec((blk, width), lambda i: (0, 0)),
            pl.BlockSpec((1, width), lambda i: (0, 0)),
        ]
        + [pl.BlockSpec((inner, width), lambda i: (0, 0)) for _ in wos],
        out_specs=[pl.BlockSpec((blk, width), lambda i: (0, 0))] * 2
        + [pl.BlockSpec((1, width), lambda i: (0, 0))]
        + [pl.BlockSpec((blk, inner), lambda i: (0, 0))] * 4,
        out_shape=(
            jax.ShapeDtypeStruct((blk, width), F32),
            jax.ShapeDtypeStruct((blk, width), BF16),
            jax.ShapeDtypeStruct((1, width), F32),
        )
        + tuple(jax.ShapeDtypeStruct((blk, inner), BF16) for _ in wos),
        cost_estimate=pl.CostEstimate(flops=8 * blk * width * inner, bytes_accessed=8 * inner * width + 16 * blk * width, transcendentals=0),
        name="back",
    )(near, got, y1, cot, gain, *wos)


def join_rows_kernel(x_ref, mine_ref, other_ref, *refs):
    out_ref = refs[-1]
    first = pl.program_id(0) == x_ref[0]

    @pl.when(first)
    def _():
        out_ref[...] = mine_ref[...].astype(F32)

    @pl.when(jnp.logical_not(first))
    def _():
        out_ref[...] = other_ref[...].astype(F32)


def join_rows(x_at, mine, other, total, part, parts, kept):
    rows, width = mine.shape
    extra = [] if kept is None else [kept]
    return pl.pallas_call(
        join_rows_kernel,
        out_shape=jax.ShapeDtypeStruct((total, width), F32),
        grid_spec=pltpu.PrefetchScalarGridSpec(
            num_scalar_prefetch=1,
            grid=(2,),
            in_specs=[pl.BlockSpec((rows, width), lambda h, x: (0, 0))] * 2 + [pl.BlockSpec(memory_space=pl.ANY) for _ in extra],
            out_specs=pl.BlockSpec((rows, width), lambda h, x: (h * parts + part, 0)),
        ),
        input_output_aliases={3: 0} if extra else {},
        cost_estimate=pl.CostEstimate(flops=0, bytes_accessed=12 * rows * width, transcendentals=0),
        name="join_rows",
    )(x_at, mine, other, *extra)


def join_cols_kernel(x_ref, mine_ref, other_ref, *refs):
    out_ref = refs[-1]
    half = mine_ref.shape[1]
    rest = out_ref.shape[1] - half
    mine, other = mine_ref[...].astype(F32), other_ref[...].astype(F32)
    first = x_ref[0] == 0
    out_ref[:, :half] = jnp.where(first, mine, other)
    out_ref[:, half:] = jnp.where(first, other, mine)[:, :rest]


def join_cols(x_at, mine, other, shape, part, parts, kept):
    rows, half = mine.shape
    sub = rows
    while sub % 16 == 0 and sub > 256:
        sub //= 2
    steps = rows // sub
    extra = [] if kept is None else [kept]
    return pl.pallas_call(
        join_cols_kernel,
        out_shape=jax.ShapeDtypeStruct(shape, F32),
        grid_spec=pltpu.PrefetchScalarGridSpec(
            num_scalar_prefetch=1,
            grid=(steps,),
            in_specs=[pl.BlockSpec((sub, half), lambda i, x: (i, 0))] * 2 + [pl.BlockSpec(memory_space=pl.ANY) for _ in extra],
            out_specs=pl.BlockSpec((sub, shape[1]), lambda i, x: (part * steps + i, 0)),
        ),
        input_output_aliases={3: 0} if extra else {},
        cost_estimate=pl.CostEstimate(flops=0, bytes_accessed=12 * rows * half, transcendentals=0),
        name="join_cols",
    )(x_at, mine, other, *extra)


def join_qkv_kernel(x_ref, mine_ref, other_ref, q_ref, k_ref, v_ref):
    picked = jnp.where(pl.program_id(0) == x_ref[0], mine_ref[...].astype(F32), other_ref[...].astype(F32))
    inner = q_ref.shape[1]
    for i, ref in enumerate((q_ref, k_ref, v_ref)):
        ref[...] = picked[:, i * inner : (i + 1) * inner]


def join_qkv(x_at, mine, other):
    rows, width = mine.shape
    inner = width // 3
    return pl.pallas_call(
        join_qkv_kernel,
        out_shape=tuple(jax.ShapeDtypeStruct((2 * rows, inner), F32) for _ in range(3)),
        grid_spec=pltpu.PrefetchScalarGridSpec(
            num_scalar_prefetch=1,
            grid=(2,),
            in_specs=[pl.BlockSpec((rows, width), lambda h, x: (0, 0))] * 2,
            out_specs=[pl.BlockSpec((rows, inner), lambda h, x: (h, 0))] * 3,
        ),
        cost_estimate=pl.CostEstimate(flops=0, bytes_accessed=12 * rows * width, transcendentals=0),
        name="join_qkv",
    )(x_at, mine, other)


def attn_backward_kernel(
    place_ref, buckets_ref, qkv_ref, grad_ref, prob_ref, gqkv_ref, gtable_ref, dk_ref, dv_ref, tiles_ref, vec_ref,
    *, heads, size, blk, nblk, bins
):
    step = pl.program_id(0)
    place = place_ref[0]
    inner = heads * size

    @pl.when(step == 0)
    def _():
        dk_ref[...] = jnp.zeros_like(dk_ref)
        dv_ref[...] = jnp.zeros_like(dv_ref)
        tiles_ref[...] = jnp.zeros_like(tiles_ref)

    here = place ^ swap_bits(step)
    rows = pl.ds(step * blk, blk)
    for h in range(heads):
        query = qkv_ref[rows, h * size : (h + 1) * size]
        keys = qkv_ref[:, inner + h * size : inner + (h + 1) * size]
        values = qkv_ref[:, 2 * inner + h * size : 2 * inner + (h + 1) * size]
        grad = grad_ref[rows, h * size : (h + 1) * size]
        prob_low = prob_ref[h]
        prob = prob_low.astype(F32)
        grad_prob = dot_nt(grad, values)
        delta = jnp.sum(prob * grad_prob, axis=1, keepdims=True)
        grad_scores = (prob * (grad_prob - delta)).astype(BF16)
        dv_ref[h] += dot_tn(prob_low, grad)
        dk_ref[h] += dot_tn(grad_scores, query)
        gqkv_ref[rows, h * size : (h + 1) * size] = dot_nn(grad_scores, keys).astype(BF16)
        for b, m in enumerate(ORDER):
            tiles_ref[h, (place ^ m) - here + nblk - 1] += grad_scores[:, b * blk : (b + 1) * blk].astype(F32)

    @pl.when(step == nblk - 1)
    def _():
        vec_ref[...] = jnp.zeros_like(vec_ref)
        back = (
            lax.broadcasted_iota(jnp.int32, (blk, blk), 0) + lax.broadcasted_iota(jnp.int32, (blk, blk), 1) == blk - 1
        ).astype(F32)
        for h in range(heads):
            gqkv_ref[:, inner + h * size : inner + (h + 1) * size] = dk_ref[h].astype(BF16)
            gqkv_ref[:, 2 * inner + h * size : 2 * inner + (h + 1) * size] = dv_ref[h].astype(BF16)
            for d in range(2 * nblk - 1):
                flip = jnp.dot(back, tiles_ref[h, d], precision=lax.Precision.HIGHEST, preferred_element_type=F32)
                wide = jnp.concatenate([flip, jnp.zeros((blk, blk), F32)], axis=1)
                moved = pltpu.roll(wide, 1, 1, stride=1, stride_axis=0)
                vec_ref[h : h + 1, d * blk : (d + 2) * blk] += jnp.sum(moved, axis=0, keepdims=True)
        pick = (lax.broadcasted_iota(jnp.int32, (bins, 1), 0) == buckets_ref[...]).astype(F32)
        gtable_ref[...] = lax.dot_general(
            pick, vec_ref[...], (((1,), (1,)), ((), ())), precision=lax.Precision.HIGHEST, preferred_element_type=F32
        )


def attn_backward(place, buckets, qkv, grad, prob, heads, size, blk, bins):
    count = qkv.shape[0]
    nblk = count // blk
    whole = lambda i, *_: (0, 0)
    return pl.pallas_call(
        functools.partial(attn_backward_kernel, heads=heads, size=size, blk=blk, nblk=nblk, bins=bins),
        out_shape=(jax.ShapeDtypeStruct(qkv.shape, BF16), jax.ShapeDtypeStruct((bins, 8), F32)),
        grid_spec=pltpu.PrefetchScalarGridSpec(
            num_scalar_prefetch=1,
            grid=(nblk,),
            in_specs=[
                pl.BlockSpec(buckets.shape, whole),
                pl.BlockSpec(qkv.shape, whole),
                pl.BlockSpec(grad.shape, whole),
                pl.BlockSpec((heads, blk, count), lambda i, *_: (0, i, 0)),
            ],
            out_specs=[pl.BlockSpec(qkv.shape, whole), pl.BlockSpec((bins, 8), whole)],
            scratch_shapes=[
                pltpu.VMEM((heads, count, size), F32),
                pltpu.VMEM((heads, count, size), F32),
                pltpu.VMEM((heads, 2 * nblk - 1, blk, blk), F32),
                pltpu.VMEM((8, 2 * nblk * blk), F32),
            ],
        ),
        cost_estimate=pl.CostEstimate(flops=10 * heads * count * count * size, bytes_accessed=4 * heads * count * count, transcendentals=0),
        name="attn_backward",
    )(place, buckets, qkv, grad, prob)


def body(
    tokens, cotangent, gain_attn, w_query, w_key, w_value, w_out, bias_table, gain_ffn, w_gate, w_up, w_down, lengths, buckets,
):
    n_t, n_d = lax.axis_size("tensor"), lax.axis_size("dp")
    blk, width = tokens.shape
    heads = bias_table.shape[1]
    inner = w_query.shape[1]
    size = inner // heads
    bins = bias_table.shape[0]
    t_at, d_at = lax.axis_index("tensor"), lax.axis_index("dp")
    x_at, z_at, n_z = d_at & 1, d_at >> 1, n_d // 2
    x_arr = x_at.astype(jnp.int32).reshape(1)
    place = t_at.astype(jnp.int32).reshape(1)
    held = [place]

    def turn(*values):
        return lax.optimization_barrier((*values, held[0]))[: len(values)]

    def ended(value):
        held[0] = value
        return value

    def tensor_swap(value, mask):
        return lax.ppermute(value, "tensor", [(i, i ^ mask) for i in range(n_t)])

    def dp_swap(value, mask):
        return lax.ppermute(value, "dp", [(i, i ^ mask) for i in range(n_d)])

    def z_send(value, pairs):
        return lax.ppermute(value, "dp", [(2 * a + x, 2 * b + x) for a, b in pairs for x in (0, 1)])

    def line_steps():
        if n_z == 4:
            at_end = (z_at == 0) | (z_at == 3)
            return [
                (lambda v: z_send(v, ((0, 1), (3, 2))), lambda v, got: v + got),
                (lambda v: z_send(v, ((1, 2), (2, 1))), lambda v, got: v + got),
                (lambda v: z_send(v, ((1, 0), (2, 3))), lambda v, got: jnp.where(at_end, got, v)),
            ]
        masks = [2 << i for i in range((n_z - 1).bit_length())]
        return [(functools.partial(lambda m, v: dp_swap(v, m), m), lambda v, got: v + got) for m in masks]

    class Chunk:
        def __init__(self, value, finish, first=()):
            self.steps = [*first, *line_steps()]
            self.value, self.finish = value, finish
            self.got = self.steps[0][0](value)

        def advance(self):
            if self.steps:
                value, got = turn(self.value, self.got)
                self.value = ended(self.steps.pop(0)[1](value, got))
                self.got = self.steps[0][0](self.value) if self.steps else dp_swap(self.value, 1)
            else:
                value, got = turn(self.value, self.got)
                ended(self.finish(value, got))
                self.finish = None

    tok_y = tensor_swap(tokens, 2)
    tok_c = tensor_swap(tokens, 1)
    tok_yc = tensor_swap(tok_y, 1)

    wo_own, cot_own = lax.optimization_barrier((w_out, cotangent, tok_y))[:2]
    wo_y = tensor_swap(wo_own, 2)
    wo_c = tensor_swap(wo_own, 1)

    def spread8(value):
        return tensor_swap(value, 2), dp_swap(value, 1)

    def spread8_rest(value, from_y, from_x):
        half = blk // 2
        diag = jnp.concatenate([tensor_swap(from_x[:half], 2), dp_swap(from_y[half:], 1)], axis=0)
        return [value, from_x, from_y, diag]

    cot_y, cot_x = spread8(cot_own)

    units = w_down.shape[0]
    half = -(-units // 256) * 128
    spare = 2 * half - units
    wg = lax.dynamic_slice_in_dim(jnp.pad(w_gate, ((0, 0), (0, spare))), x_at * half, half, 1)
    wu = lax.dynamic_slice_in_dim(jnp.pad(w_up, ((0, 0), (0, spare))), x_at * half, half, 1)
    wd = lax.dynamic_slice_in_dim(jnp.pad(w_down, ((0, spare), (0, 0))), x_at * half, half, 0)

    bucket_row = jnp.pad(buckets, (1, 0), constant_values=-1).reshape(1, -1)
    gain_1, gain_2 = gain_attn.reshape(1, -1), gain_ffn.reshape(1, -1)
    n1, qkv, prob, *attns = front(
        place, lengths, bias_table, bucket_row, gain_1, (tokens, tok_y, tok_c, tok_yc), w_query, w_key, w_value, heads, size
    )

    def to_owners(blocks):
        return [blocks[0]] + [tensor_swap(blocks[b], ORDER[b]) for b in range(1, n_t)]

    mine = to_owners(attns)
    wo_yc = tensor_swap(wo_y, 1)
    wos = [w_out, wo_y, wo_c, wo_yc]
    y1, n2 = middle(mine, wos, tokens, gain_2)
    n2_y, n2_x = spread8(n2)
    cot_near = jnp.concatenate(spread8_rest(cotangent, cot_y, cot_x), axis=0)
    cot_all = jnp.concatenate([cot_near, tensor_swap(cot_near, 1)], axis=0)
    near = spread8_rest(n2, n2_y, n2_x)
    blocks = near + [tensor_swap(b, 1) for b in near]
    hidden, gg, gu, n2_all = ffn(blocks, cot_all, wg, wu, wd)

    held[0] = hidden
    outs = {}
    chunks = []

    def rows_finish(name, total, part, parts):
        def finish(mine, other):
            outs[name] = join_rows(x_arr, mine, other, total, part, parts, outs.get(name))
            return outs[name]

        return finish

    def cols_finish(name, shape, part, parts):
        def finish(mine, other):
            outs[name] = join_cols(x_arr, mine, other, shape, part, parts, outs.get(name))
            return outs[name]

        return finish

    def launch(value, make, parts):
        rows = value.shape[0] // parts
        for i in range(parts):
            chunks.append(Chunk(value[i * rows : (i + 1) * rows], make(i)))

    side = n_t * blk
    parts = 2

    g_down = ended(dot_tn(*turn(hidden, cot_all)).astype(BF16))
    launch(g_down, lambda i: rows_finish("down", units, i, parts), parts)

    gg_t, gu_t = turn(gg, gu)
    gn2_far = ended((dot_nt(gg_t[side:], wg) + dot_nt(gu_t[side:], wu)).astype(BF16))
    gn2_c = tensor_swap(gn2_far, 1)
    g_gate = ended(dot_tn(*turn(n2_all, gg)).astype(BF16))
    launch(g_gate, lambda i: cols_finish("gate", w_gate.shape, i, parts), parts)
    gg_t, gu_t = turn(gg, gu)
    gn2_near = ended((dot_nt(gg_t[:side], wg) + dot_nt(gu_t[:side], wu)).astype(BF16))
    gn2_near, gn2_c = turn(gn2_near, gn2_c)
    gn2_near = ended(gn2_near + gn2_c)
    gn2_y = tensor_swap(gn2_near[2 * blk :], 2)
    g_up = ended(dot_tn(*turn(n2_all, gu)).astype(BF16))
    launch(g_up, lambda i: cols_finish("up", w_up.shape, i, parts), parts)
    (hid,) = turn(hidden)
    ffn_far = ended(dot_nn(hid[side:], wd).astype(BF16))
    ffn_c = tensor_swap(ffn_far, 1)

    chunks[0].advance()

    (hid,) = turn(hidden)
    ffn_near = ended(dot_nn(hid[:side], wd).astype(BF16))
    ffn_near, ffn_c = turn(ffn_near, ffn_c)
    ffn_near = ended(ffn_near + ffn_c)
    gn2_near, gn2_y = turn(gn2_near, gn2_y)
    gn2_near = ended(gn2_near[: 2 * blk] + gn2_y)
    gn2_x = dp_swap(gn2_near[blk:], 1)
    ffn_y = tensor_swap(ffn_near[2 * blk :], 2)

    chunks[1].advance()
    chunks[0].advance()

    near_b, got_b = turn(gn2_near, gn2_x)
    gy1, gy_low, gain2_part, *gas = back(near_b[:blk], got_b, y1, cotangent, gain_2, wos)
    ended(gy_low)
    gas = to_owners(gas)
    gy_y = tensor_swap(gy_low, 2)

    chunks[2].advance()
    chunks[1].advance()
    chunks[0].advance()

    gas = turn(*gas)
    ga = jnp.concatenate(gas, axis=0)
    gqkv, gtable = attn_backward(place, bucket_row, qkv, ga, prob, heads, size, blk, bins)
    ended(gqkv)

    def full_chunk(value, finish):
        rows = value.shape[0] // 2
        give = lax.dynamic_slice_in_dim(value, (1 - x_at) * rows, rows, 0)
        keep = lax.dynamic_slice_in_dim(value, x_at * rows, rows, 0)
        chunk = Chunk.__new__(Chunk)
        chunk.steps = [(None, lambda v, got: v + got), *line_steps()]
        chunk.value, chunk.finish = keep, finish
        chunk.got = dp_swap(give, 1)
        return chunk

    def qkv_finish(mine, other):
        outs["qkv"] = join_qkv(x_arr, mine, other)
        return outs["qkv"][0]

    gqkv_t, n1_t = turn(gqkv, n1)
    g_qkv = ended(dot_tn(n1_t, gqkv_t).astype(BF16))
    chunk_qkv = full_chunk(g_qkv, qkv_finish)
    gy_own, gy_y = turn(gy_low, gy_y)
    gy_near = ended(jnp.concatenate([gy_own, gy_y], axis=0))
    gy_far = tensor_swap(gy_near, 1)

    w_qkv = jnp.concatenate([w_query, w_key, w_value], axis=1)
    (gqkv_t,) = turn(gqkv)
    gn1_far = ended(dot_nt(gqkv_t[2 * blk :], w_qkv).astype(BF16))
    gn1_c = tensor_swap(gn1_far, 1)

    chunks[3].advance()
    chunks[2].advance()
    chunks[1].advance()
    chunks[0].advance()

    gy_near, gy_far = turn(gy_near, gy_far)
    gy_all = jnp.concatenate([gy_near, gy_far], axis=0)
    attn = jnp.concatenate(attns, axis=0)
    g_wo = ended(dot_tn(attn, gy_all).astype(BF16))
    chunk_wo = full_chunk(g_wo, rows_finish("out", 2 * (g_wo.shape[0] // 2), 0, 1))

    (gqkv_t,) = turn(gqkv)
    gn1_near = ended(dot_nt(gqkv_t[: 2 * blk], w_qkv).astype(BF16))
    gn1_near, gn1_c = turn(gn1_near, gn1_c)
    gn1_near = ended(gn1_near + gn1_c)
    gn1_y = tensor_swap(gn1_near[blk:], 2)

    ffn_near, ffn_y = turn(ffn_near, ffn_y)
    ffn_near = ended(ffn_near[: 2 * blk] + ffn_y)
    ffn_x = dp_swap(ffn_near[blk:], 1)

    chunks[4].advance()
    chunk_qkv.advance()
    chunks[3].advance()
    chunks[2].advance()
    chunks[1].advance()

    gn1_near, gn1_y = turn(gn1_near, gn1_y)
    gn1 = gn1_near[:blk].astype(F32) + gn1_y.astype(F32)
    tok = tokens.astype(F32)
    rr1 = lax.rsqrt(jnp.mean(tok * tok, axis=1, keepdims=True) + 1e-6)
    gain1_part = jnp.sum(gn1 * tok * rr1, axis=0)
    c1 = gn1 * gain_attn
    grad_tokens = (gy1 + rr1 * c1 - tok * (rr1 * rr1 * rr1) * jnp.mean(c1 * tok, axis=1, keepdims=True)).astype(BF16)
    small = jnp.concatenate([gain1_part, gain2_part.reshape(-1)])
    smalls = [functools.partial(lambda m, v: tensor_swap(v, m), 1 << i) for i in range((n_t - 1).bit_length())]
    smalls += [functools.partial(lambda m, v: dp_swap(v, m), 1 << i) for i in range((n_d - 1).bit_length())]
    n_small = (n_t - 1).bit_length()
    ended(grad_tokens)

    def small_step():
        nonlocal small
        if smalls:
            if len(smalls) == (n_d - 1).bit_length():
                small = jnp.concatenate([small, gtable.reshape(-1)])
            (small,) = turn(small)
            small = small + smalls.pop(0)(small)
            ended(small)

    ffn_near, ffn_x = turn(ffn_near, ffn_x)
    block_out = ended((y1 + ffn_near[:blk].astype(F32) + ffn_x.astype(F32)).astype(BF16))

    chunks.append(chunk_wo)
    chunks.append(chunk_qkv)
    chunk_wo.advance()
    small_step()
    chunks[5].advance()
    chunks[4].advance()
    chunks[3].advance()
    chunks[2].advance()
    small_step()
    live = [c for c in chunks if c.finish is not None]
    while live:
        for c in sorted(live, key=lambda c: -len(c.steps)):
            c.advance()
        small_step()
        live = [c for c in chunks if c.finish is not None]
    while smalls:
        small_step()

    gain1_sum, gain2_sum = small[:width], small[width : 2 * width]
    table_sum = small[2 * width :].reshape(gtable.shape)[:, :heads]

    return (
        block_out,
        grad_tokens,
        gain1_sum,
        *outs["qkv"],
        outs["out"],
        table_sum,
        gain2_sum,
        outs["gate"],
        outs["up"],
        outs["down"],
    )


def solution(mesh):
    rows, cols, both = P("tensor", None), P(None, "tensor"), P(("dp", "tensor"), None)
    return jax.shard_map(
        body,
        mesh=mesh,
        in_specs=(both, both, P(), cols, cols, cols, rows, cols, P(), cols, cols, rows, P("dp", None), P()),
        out_specs=(both, both, P(), cols, cols, cols, rows, cols, P(), cols, cols, rows),
        check_vma=False,
    )
```
